32 devices in a mesh: enc: 8 (over z, x), section: 2 (over core), llmdp: 2 (over y).
Axes of the slice: x: 2, y: 2, z: 4, core: 2. Of those that a mesh axis runs over, the one named last changes fastest.
Arguments:
- patches: bfloat16 [2048, 3200], P('enc', ('section', 'llmdp')), may hold values from -6 to 6
- gain: float32 [3200], replicated, may hold values from 0.25 to 1.75
- shift: float32 [3200], replicated, may hold values from -3 to 3
- proj_weight: bfloat16 [3200, 8192], P('enc', ('section', 'llmdp')), may hold values from -0.109375 to 0.109375
- llm_rank: int32 [2048, 1], P('enc'), may hold values from 0 to 7; in each aligned block of 256 rows (0 to 255, 256 to 511, ...) at most 96 rows name the same one
- embed_grad: bfloat16 [6144, 8192], P('enc', ('section', 'llmdp')), may hold values from -0.59765625 to 0.59765625
Outputs:
- embeds_recv: bfloat16 [6144, 8192], P('enc', ('section', 'llmdp'))
- hidden_state_gradient: bfloat16 [2048, 3200], P('enc', ('section', 'llmdp'))
- grad_weight: float32 [3200, 8192], P('enc', ('section', 'llmdp'))
- gain_gradient: float32 [3200], P(('section', 'llmdp'))
- grad_shift: float32 [3200], P(('section', 'llmdp'))
The draws below stay inside these ranges and needn't reach their ends.
Inputs may be any that keep to these rules, and one draw needn't show every extreme that they name: `llm_rank`: among the 256 rows of one device, at most 96 name the same owner, a bound that some block reaches.
All inputs are finite; a program needn't handle non-finite values.
Results may differ from the reference program's by a relative error of at most 0.018.
Values may be sent and summed in bfloat16 or wider, within the bound.
A program may use at most 128 MiB of HBM per device.

```python
import math
import jax
import jax.numpy as jnp
import numpy as np
from jax import lax

D = 3200
E = 8192
TOK_DEV = 256
TOKENS = 2048
MOST = 96
RECV = 6144
N_ENC = 8
N_SECTION = 2
N_LLMDP = 2


def level_of(own_key, shape, split, least, largest):
    factor_of = 1.0
    for axis_at, blocks in split:
        steps = jax.random.uniform(jax.random.fold_in(jax.random.fold_in(own_key, 6), axis_at), (blocks,), jnp.float32, least / len(split), largest / len(split))
        factor_of = factor_of * jnp.repeat(jnp.exp(steps), shape[axis_at] // blocks).reshape((-1,) + (1,) * (len(shape) - 1 - axis_at))
    return factor_of


def shared_out(stream_key, own, number, rows, count, top, limit, lean):
    order = jax.random.permutation(stream_key, count)
    heavy_load, common = portions_of(count, rows * top, limit, lean, True), portions_of(count, rows * top, limit, lean, False)
    places = jnp.arange(count)

    def named(sizes, turn):
        used = int((sizes > 0).sum())
        fixed = max(1, used // 4)
        moved = fixed + (places - fixed + turn * (used - fixed)) % max(1, count - fixed)
        return jnp.zeros((count,), jnp.int32).at[order[jnp.where(places < fixed, places, moved)]].set(jnp.asarray(sizes, jnp.int32))

    sizes = jnp.where(number % 4 == 0, named(heavy_load, number // 4), named(common, number - number // 4 - 1))
    mixed = jax.random.permutation(jax.random.fold_in(own, 3), count)
    source_of, receiver = mixed[0:count // 2 * 2:2], mixed[1:count // 2 * 2:2]
    slack = jnp.minimum(sizes[source_of] - 1, limit - sizes[receiver]) // 2
    slack = jnp.where((source_of == order[0]) | (receiver == order[0]) | (sizes[receiver] == 0), 0, jnp.maximum(slack, 0))
    moved = jax.random.randint(jax.random.fold_in(own, 4), (count // 2,), 0, 1 << 20) % (slack + 1)
    sizes = sizes.at[source_of].add(-moved).at[receiver].add(moved)
    labels = jnp.searchsorted(jnp.cumsum(sizes), jnp.arange(rows * top), side="right").astype(jnp.int32)
    listing = labels.reshape(top, rows).T
    listing = listing[jax.random.permutation(jax.random.fold_in(own, 1), rows)]
    turn = jax.random.randint(jax.random.fold_in(own, 2), (rows, 1), 0, top)
    return jnp.take_along_axis(listing, (jnp.arange(top)[None, :] + turn) % top, axis=1)


def portions_of(count, total, reach, slope, full):
    weights = [(1 << 20) // math.isqrt(grade ** slope) + 1 for grade in range(1, count + 1)]
    largest = reach if full else min(reach, max(-(-total // count), total * weights[0] // sum(weights)))
    least = 1 if total - largest >= count - 1 else 0
    counts, spare = [largest] + [least] * (count - 1), total - largest - least * (count - 1)
    while spare > 0:
        movable = [i for i in range(1, count) if counts[i] < largest] or [i for i in range(1, count) if counts[i] < reach]
        whole, remaining = sum([weights[i] for i in movable]), spare
        for i in movable:
            more = min(reach - counts[i], max(1, remaining * weights[i] // whole), spare)
            counts[i] = counts[i] + more
            spare = spare - more
    return np.array(counts)


def noise(own_key, extent, scale, most, pieces=(), held_as=jnp.bfloat16):
    factor_of = level_of(own_key, extent, pieces, -0.22, 0.18) if pieces else 1.0
    array = jax.random.normal(own_key, extent, jnp.float32) * scale * factor_of
    return jnp.minimum(jnp.maximum(array, -most), most).astype(held_as)


def setup_inputs(seed: int = 0) -> dict:
    arg_keys = jax.random.split(jax.random.key(seed), 7)
    patches = noise(arg_keys[0], (TOKENS, D), 1.0, 6.0, ((0, 8), (1, 4)))
    gain = jnp.clip(1.0 + 0.15 * jax.random.normal(arg_keys[1], (D,), jnp.float32), 0.25, 1.75)
    shift = noise(arg_keys[2], (D,), 0.5, 3.0, (), jnp.float32)
    proj_weight = noise(arg_keys[3], (D, E), D ** -0.5, 0.109375, ((0, 8), (1, 4)))
    llm_rank_keys = jax.random.split(jax.random.fold_in(arg_keys[4], 1), TOKENS // TOK_DEV)
    llm_rank_turns = jax.random.permutation(jax.random.fold_in(arg_keys[4], 3), TOKENS // TOK_DEV)
    llm_rank = jax.vmap(lambda own, number: shared_out(jax.random.fold_in(arg_keys[4], 2), own, number, TOK_DEV, N_ENC, 1, MOST, 2))(llm_rank_keys, llm_rank_turns).reshape((TOKENS, 1))
    embed_grad = noise(arg_keys[5], (RECV, E), 0.1, 0.59765625, ((0, 8), (1, 4)))
    return {"patches": patches, "gain": gain, "shift": shift, "proj_weight": proj_weight, "llm_rank": llm_rank, "embed_grad": embed_grad}


EPSILON = 1e-05

def reference(patches, gain, shift, proj_weight, llm_rank, embed_grad):
    value_entries = patches.astype(jnp.float32)
    row_average = lax.optimization_barrier(jnp.mean(value_entries, 1, keepdims=True))
    variance = lax.optimization_barrier(jnp.mean(value_entries * value_entries, 1, keepdims=True)) - row_average * row_average
    inverse_deviation = lax.rsqrt(variance + EPSILON)
    standardized_rows = (value_entries - row_average) * inverse_deviation
    normed_hidden = (standardized_rows * gain + shift).astype(jnp.bfloat16)
    embed = jnp.dot(normed_hidden, proj_weight, preferred_element_type=jnp.float32).astype(jnp.bfloat16)
    target = llm_rank[:, 0].astype(jnp.int32).reshape(N_ENC, TOK_DEV)
    owners = jnp.arange(N_ENC, dtype=jnp.int32)
    hits = (target[:, :, None] == owners[None, None, :]).astype(jnp.int32)
    rank = lax.optimization_barrier(jnp.sum((jnp.cumsum(hits, 1) - hits) * hits, 2)).astype(jnp.int32)
    slot = (target * (N_ENC * MOST) + owners[:, None] * MOST + rank).reshape(-1).astype(jnp.int32)
    embeds_recv = jnp.zeros((RECV, E), jnp.bfloat16).at[slot].set(embed)
    d_embed = embed_grad[slot]
    groups = N_SECTION * N_LLMDP
    group_cols = E // groups

    def group_step(total, index):
        start = (index * group_cols).astype(jnp.int32)
        grad_part = lax.dynamic_slice_in_dim(d_embed, start, group_cols, 1)
        weight_part = lax.dynamic_slice_in_dim(proj_weight, start, group_cols, 1)
        term = lax.dot_general(grad_part, weight_part, (((1,), (1,)), ((), ())), preferred_element_type=jnp.float32)
        return (total + lax.optimization_barrier(term.astype(jnp.bfloat16)).astype(jnp.float32), None)
    normalized_gradient, _ = lax.scan(group_step, jnp.zeros((TOKENS, D), jnp.float32), jnp.arange(groups, dtype=jnp.int32))

    def block_step(total, pair):
        term = lax.dot_general(pair[0], pair[1], (((0,), (0,)), ((), ())), preferred_element_type=jnp.float32)
        return (total + lax.optimization_barrier(term.astype(jnp.bfloat16)).astype(jnp.float32), None)
    grad_weight, _ = lax.scan(block_step, jnp.zeros((D, E), jnp.float32), (normed_hidden.reshape(N_ENC, TOK_DEV, D), d_embed.reshape(N_ENC, TOK_DEV, E)))
    centered_gradient = normalized_gradient * gain
    gradient_row_average = lax.optimization_barrier(jnp.mean(centered_gradient, 1, keepdims=True))
    gradient_cross_product = lax.optimization_barrier(jnp.mean(centered_gradient * standardized_rows, 1, keepdims=True))
    hidden_state_gradient = (inverse_deviation * (centered_gradient - gradient_row_average - standardized_rows * gradient_cross_product)).astype(jnp.bfloat16)
    gain_gradient = lax.optimization_barrier(jnp.sum(normalized_gradient * standardized_rows, 0))
    grad_shift = lax.optimization_barrier(jnp.sum(normalized_gradient, 0))
    return (embeds_recv, hidden_state_gradient, grad_weight, gain_gradient, grad_shift)
```

```python
import jax
import jax.numpy as jnp
from jax import lax
from jax.sharding import PartitionSpec as P

EPSILON = 1e-05


MAX_BLOCK = 2


def block_size(senders, out_cols):
    size = MAX_BLOCK
    while size > 1 and (senders % size or senders == size or out_cols % (size * 128)):
        size //= 2
    return size


def body(patches, gain, shift, proj_weight, llm_rank, embed_grad):
    features = ("section", "llmdp")
    own_rows, owned_width = patches.shape
    width = gain.shape[0]
    weight_rows, out_cols = proj_weight.shape
    senders = lax.axis_size("enc")
    block = block_size(senders, out_cols)
    near = [[b * block + i for i in range(block)] for b in range(senders // block)]
    far = [[b * block + i for b in range(senders // block)] for i in range(block)]

    def near_exchange(x, split, concat):
        return lax.all_to_all(x, "enc", split, concat, axis_index_groups=near, tiled=True)

    column_start = lax.axis_index(features) * owned_width
    gain_own = lax.dynamic_slice_in_dim(gain, column_start, owned_width, 0)

    weight_part = near_exchange(proj_weight, 1, 0)
    weight = lax.all_gather(weight_part, "enc", axis=0, axis_index_groups=far, tiled=True)

    block_rows = lax.all_gather(patches, "enc", axis=0, axis_index_groups=near, tiled=True)
    complete_rows = lax.all_gather(block_rows, features, axis=1, tiled=True).astype(jnp.float32)
    row_average = jnp.mean(complete_rows, 1, keepdims=True)
    variance = jnp.mean(complete_rows * complete_rows, 1, keepdims=True) - row_average * row_average
    inverse_deviation = lax.rsqrt(variance + EPSILON)
    standardized = (complete_rows - row_average) * inverse_deviation
    normed = (standardized * gain + shift).astype(jnp.bfloat16)

    row_start = (lax.axis_index("enc") % block) * own_rows
    average_own = lax.dynamic_slice_in_dim(row_average, row_start, own_rows, 0)
    deviation_own = lax.dynamic_slice_in_dim(inverse_deviation, row_start, own_rows, 0)
    standardized_owned = (patches.astype(jnp.float32) - average_own) * deviation_own

    most_slots = embed_grad.shape[0] // senders
    target = llm_rank[:, 0]
    owners = jnp.arange(senders, dtype=jnp.int32)
    hits = (target[:, None] == owners[None, :]).astype(jnp.int32)
    rank = jnp.sum((jnp.cumsum(hits, 0) - hits) * hits, 1)
    slot = target * most_slots + rank

    def enc_exchange(x):
        return lax.all_to_all(
            x.reshape(senders, most_slots, out_cols), "enc", split_axis=0, concat_axis=0, tiled=True
        ).reshape(senders * most_slots, out_cols)

    d_embed = near_exchange(enc_exchange(embed_grad)[slot], 1, 0)
    grad_part = lax.psum_scatter(
        lax.dot_general(
            normed, d_embed, (((0,), (0,)), ((), ())), preferred_element_type=jnp.float32
        ).astype(jnp.bfloat16),
        "enc",
        scatter_dimension=0,
        axis_index_groups=far,
        tiled=True,
    )
    grad_weight = near_exchange(grad_part, 0, 1).astype(jnp.float32)

    embed_part = jnp.dot(normed, weight, preferred_element_type=jnp.float32).astype(jnp.bfloat16)
    embed = near_exchange(embed_part, 0, 1)
    outgoing = jnp.zeros((senders * most_slots, out_cols), jnp.bfloat16).at[slot].set(embed)
    embeds_recv = enc_exchange(outgoing)

    partial_grad = lax.dot_general(
        d_embed, weight, (((1,), (1,)), ((), ())), preferred_element_type=jnp.float32
    )
    group_count = width // owned_width
    pieces = partial_grad.astype(jnp.bfloat16).reshape(block * own_rows, group_count, owned_width)
    columns = lax.all_to_all(pieces, features, split_axis=1, concat_axis=1, tiled=True)
    column_sum = jnp.sum(columns.astype(jnp.float32), 1).astype(jnp.bfloat16)
    shares = near_exchange(column_sum.reshape(block, own_rows, owned_width), 0, 0)
    owned_normalized_gradient = jnp.sum(shares.astype(jnp.float32), 0)
    owned_centered_gradient = owned_normalized_gradient * gain_own
    mean_sum, cross_sum = lax.psum(
        (
            jnp.sum(owned_centered_gradient, 1),
            jnp.sum(owned_centered_gradient * standardized_owned, 1),
        ),
        features,
    )
    gradient_row_average = (mean_sum / width)[:, None]
    gradient_cross_product = (cross_sum / width)[:, None]
    hidden_state_gradient = (
        deviation_own
        * (
            owned_centered_gradient
            - gradient_row_average
            - standardized_owned * gradient_cross_product
        )
    ).astype(jnp.bfloat16)
    gain_gradient, grad_shift = lax.psum(
        (
            jnp.sum(owned_normalized_gradient * standardized_owned, 0),
            jnp.sum(owned_normalized_gradient, 0),
        ),
        "enc",
    )
    return (embeds_recv, hidden_state_gradient, grad_weight, gain_gradient, grad_shift)


def solution(mesh):
    in_specs = (
        P("enc", ("section", "llmdp")),
        P(),
        P(),
        P("enc", ("section", "llmdp")),
        P("enc", None),
        P("enc", ("section", "llmdp")),
    )
    out_specs = (
        P("enc", ("section", "llmdp")),
        P("enc", ("section", "llmdp")),
        P("enc", ("section", "llmdp")),
        P(("section", "llmdp")),
        P(("section", "llmdp")),
    )
    return jax.shard_map(body, mesh=mesh, in_specs=in_specs, out_specs=out_specs, check_vma=False)
```
